32 devices in a mesh: dp: 8 (over y, x, core), tensor: 4 (over z).
Axes of the slice: x: 2, y: 2, z: 4, core: 2. Of those that a mesh axis runs over, the one named last changes fastest.
Arguments:
- tokens: bfloat16 [128, 5376], P('dp'), may hold values from -6 to 6
- lengths: int32 [128], P('dp'), may hold values from 1 to 1024, as said below
- positions: int32 [128], P('dp'), may hold values from 1 to 33791, as said below
- in_gain: float32 [5376], replicated, may hold values from 0.25 to 1.75
- q_weight: bfloat16 [5376, 4096], P('dp', 'tensor'), may hold values from -0.078125 to 0.078125
- k_weight: bfloat16 [5376, 2048], P('dp', 'tensor'), may hold values from -0.078125 to 0.078125
- v_weight: bfloat16 [5376, 2048], P('dp', 'tensor'), may hold values from -0.078125 to 0.078125
- q_gain: float32 [128], replicated, may hold values from 0.1 to 1.9
- k_gain: float32 [128], replicated, may hold values from 0.1 to 1.9
- key_cache: bfloat16 [128, 1024, 2048], P('dp', None, 'tensor'), may hold values from -480 to 480
- value_cache: bfloat16 [128, 1024, 2048], P('dp', None, 'tensor'), may hold values from -6 to 6
- out_weight: bfloat16 [4096, 5376], P('tensor', 'dp'), may hold values from -0.09375 to 0.09375
- post_gain: float32 [5376], replicated, may hold values from 0.25 to 1.75
Outputs:
- hidden_out: bfloat16 [128, 5376], P('dp')
- new_keys: bfloat16 [128, 2048], P('dp', 'tensor')
- new_values: bfloat16 [128, 2048], P('dp', 'tensor')
The draws below stay inside these ranges and needn't reach their ends.
Inputs may be any that keep to these rules, and one draw needn't show every extreme that they name: Slots 0 to lengths - 1 of a sequence hold its cache; some sequence has exactly 1024. `positions`: each position is at least the sequence's length.
All inputs are finite; a program needn't handle non-finite values.
Results may differ from the reference program's by a relative error of at most 0.012.
The reference program's roundings to bfloat16 on the way count: a program that leaves them out, or rounds other values in their place, can miss the bound.
Values may be sent and summed in bfloat16 or wider, within the bound.
A program may use at most 64 MiB of HBM per device.

```python
import jax
import jax.numpy as jnp
from jax import lax

D = 5376
H = 32
KV = 16
HD = 128
QPRE = 168
BSEQ = 16
CTX = 1024
BATCH = 128


def length_table(key):
    groups = BATCH // BSEQ
    key_one, key_two, key_three, key_four = jax.random.split(jax.random.fold_in(key, 7), 4)
    ceiling = jax.random.randint(key_one, (groups, 1), max(CTX // 8, 1), CTX + 1)
    raw_draws = jax.random.randint(key_two, (groups, BSEQ), 0, 1 << 30)
    filled = (1 + raw_draws % ceiling).reshape(BATCH)
    chosen = jax.random.randint(key_three, (), 0, BATCH)
    filled = jnp.where(jnp.arange(BATCH) == chosen, CTX, filled)
    shifts = jax.random.randint(key_four, (BATCH,), 0, 32768)
    return (filled.astype(jnp.int32), (filled + shifts).astype(jnp.int32))


def draw_lengths(key, part):
    return length_table(key)[0]


def draw_positions(key, part):
    return length_table(key)[1]


def draw_key_cache(key, part):
    key_one, key_two = jax.random.split(jax.random.fold_in(key, 13))
    normal = 3.0 * jax.random.truncated_normal(key_one, -4.0, 4.0, (BATCH, CTX, KV * HD), jnp.float32)
    return normal.astype(jnp.bfloat16)


def steps_of(stream_key, shape, cuts, least, top_value):
    level = 1.0
    for axis_at, blocks in cuts:
        heights = jax.random.uniform(jax.random.fold_in(jax.random.fold_in(stream_key, 6), axis_at), (blocks,), jnp.float32, least / len(cuts), top_value / len(cuts))
        level = level * jnp.repeat(jnp.exp(heights), shape[axis_at] // blocks).reshape((-1,) + (1,) * (len(shape) - 1 - axis_at))
    return level


def noise(key, extent, width, limit, shards=(), held_as=jnp.bfloat16):
    entries = width * jax.random.normal(key, extent, jnp.float32)
    if shards:
        entries = entries * steps_of(key, extent, shards, -0.22, 0.18)
    return jnp.clip(entries, -limit, limit).astype(held_as)


def setup_inputs(seed: int = 0) -> dict:
    arg_keys = jax.random.split(jax.random.key(seed), 14)
    tokens = noise(arg_keys[0], (BATCH, D), 1.0, 6.0, ((0, 8),))
    lengths = draw_lengths(jax.random.fold_in(arg_keys[13], 71), 0)
    positions = draw_positions(jax.random.fold_in(arg_keys[13], 71), 0)
    in_gain = jnp.clip(1.0 + 0.15 * jax.random.normal(arg_keys[3], (D,), jnp.float32), 0.25, 1.75)
    q_weight = noise(arg_keys[4], (D, H * HD), D ** -0.5, 0.078125, ((0, 8), (1, 4)))
    k_weight = noise(arg_keys[5], (D, KV * HD), D ** -0.5, 0.078125, ((0, 8), (1, 4)))
    v_weight = noise(arg_keys[6], (D, KV * HD), D ** -0.5, 0.078125, ((0, 8), (1, 4)))
    q_gain = jnp.clip(1.0 + 0.18 * jax.random.normal(arg_keys[7], (HD,), jnp.float32), 0.1, 1.9)
    k_gain = jnp.clip(1.0 + 0.18 * jax.random.normal(arg_keys[8], (HD,), jnp.float32), 0.1, 1.9)
    key_cache = draw_key_cache(jax.random.fold_in(arg_keys[13], 71), 0)
    value_cache = noise(arg_keys[10], (BATCH, CTX, KV * HD), 1.0, 6.0, ((0, 8), (2, 4)))
    out_weight = noise(arg_keys[11], (H * HD, D), (H * HD) ** -0.5, 0.09375, ((0, 4), (1, 8)))
    post_gain = jnp.clip(1.0 + 0.15 * jax.random.normal(arg_keys[12], (D,), jnp.float32), 0.25, 1.75)
    return dict(tokens=tokens, lengths=lengths, positions=positions, in_gain=in_gain, q_weight=q_weight, k_weight=k_weight, v_weight=v_weight, q_gain=q_gain, k_gain=k_gain, key_cache=key_cache, value_cache=value_cache, out_weight=out_weight, post_gain=post_gain)


epsilon = 1e-06
rope_base = 1000000.0
rope_factor = 8.0

def rms_scale(vectors, gain):
    mean_square = lax.optimization_barrier(jnp.mean(vectors * vectors, axis=-1, keepdims=True))
    return vectors * lax.rsqrt(mean_square + epsilon) * gain

def rotate(vectors, positions):
    half_width = vectors.shape[-1] // 2
    exponent = jnp.arange(half_width, dtype=jnp.float32) * (2.0 / vectors.shape[-1])
    frequency = jnp.power(rope_base, -exponent)
    angles = (positions.astype(jnp.float32) / rope_factor)[:, None] * frequency[None, :]
    cos_part = jnp.cos(angles)[:, None, :]
    sin_part = jnp.sin(angles)[:, None, :]
    first_half = vectors[..., :half_width]
    second_half = vectors[..., half_width:]
    return jnp.concatenate([first_half * cos_part - second_half * sin_part, second_half * cos_part + first_half * sin_part], axis=-1)

def reference(tokens, lengths, positions, in_gain, q_weight, k_weight, v_weight, q_gain, k_gain, key_cache, value_cache, out_weight, post_gain):
    batch_size = tokens.shape[0]
    per_group = H // KV
    normed = rms_scale(tokens.astype(jnp.float32), in_gain).astype(jnp.bfloat16)
    q_raw = jnp.dot(normed, q_weight, preferred_element_type=jnp.float32).reshape(batch_size, H, HD)
    k_raw = jnp.dot(normed, k_weight, preferred_element_type=jnp.float32).reshape(batch_size, KV, HD)
    v_raw = jnp.dot(normed, v_weight, preferred_element_type=jnp.float32)
    new_values = v_raw.astype(jnp.bfloat16)
    queries = (rotate(rms_scale(q_raw, q_gain), positions) * QPRE ** (-0.5)).astype(jnp.bfloat16)
    new_keys = rotate(rms_scale(k_raw, k_gain), positions).astype(jnp.bfloat16).reshape(batch_size, KV * HD)

    def attend(sequence):
        query_row, key_own, value_own, cache_keys, cache_values, length = sequence
        grouped = query_row.astype(jnp.float32).reshape(KV, per_group, HD)
        keys_f = cache_keys.astype(jnp.float32).reshape(CTX, KV, HD)
        values_f = cache_values.astype(jnp.float32).reshape(CTX, KV, HD)
        scores = jnp.einsum('grd,jgd->grj', grouped, keys_f)
        usable = jnp.arange(CTX) < length
        scores = jnp.where(usable[None, None, :], scores, -jnp.inf)
        self_score = jnp.einsum('grd,gd->gr', grouped, key_own.astype(jnp.float32).reshape(KV, HD))
        largest = jnp.maximum(lax.optimization_barrier(jnp.max(scores, axis=-1)), self_score)
        weights = jnp.exp(scores - largest[..., None])
        self_weight = jnp.exp(self_score - largest)
        running = lax.optimization_barrier(jnp.sum(weights, axis=-1)) + self_weight
        rounded = lax.optimization_barrier(weights.astype(jnp.bfloat16)).astype(jnp.float32)
        rounded_self = lax.optimization_barrier(self_weight.astype(jnp.bfloat16)).astype(jnp.float32)
        mixture = jnp.einsum('grj,jgd->grd', rounded, values_f)
        mixture = mixture + rounded_self[..., None] * value_own.astype(jnp.float32).reshape(KV, 1, HD)
        return (mixture / running[..., None]).reshape(H * HD).astype(jnp.bfloat16)
    attended = lax.map(attend, (queries, new_keys, new_values, key_cache, value_cache, lengths))
    projected = jnp.dot(attended, out_weight, preferred_element_type=jnp.float32)
    hidden_out = (tokens.astype(jnp.float32) + rms_scale(projected, post_gain)).astype(jnp.bfloat16)
    return (hidden_out, new_keys, new_values)
```

```python
import functools

import jax
import jax.numpy as jnp
from jax import lax
from jax.experimental import pallas as pl
from jax.experimental.pallas import tpu as pltpu
from jax.sharding import PartitionSpec as P

HD = 128
QPRE = 168
SLOTS = 256

epsilon = 1e-06
rope_base = 1000000.0
rope_factor = 8.0

MESH = pl.DeviceIdType.MESH
VMEM = pltpu.VMEM
F32 = jnp.float32
BF16 = jnp.bfloat16


def project_kernel(
    n, tok_ref, gain_ref, cos_ref, sin_ref, qg_ref, kg_ref, wq_ref, wk_ref, wv_ref,
    q_out, kx_out, vx_out, nk_out, nv_out,
    w, sbuf, rbuf, psend, precv, wsem, s1, r1, s2, r2,
):
    me = lax.axis_index("dp")
    rows, width = tok_ref.shape
    depth = wq_ref.shape[0]
    qc, kc = wq_ref.shape[1], wk_ref.shape[1]
    cols = qc + 2 * kc
    chunk = min(512, cols)
    chunks = cols // chunk

    loads = [
        pltpu.make_async_copy(wq_ref, w.at[:, pl.ds(0, qc)], wsem.at[0]),
        pltpu.make_async_copy(wk_ref, w.at[:, pl.ds(qc, kc)], wsem.at[1]),
        pltpu.make_async_copy(wv_ref, w.at[:, pl.ds(qc + kc, kc)], wsem.at[2]),
    ]
    for load in loads:
        load.start()
    barrier = pltpu.get_barrier_semaphore()
    for o in range(1, n):
        pl.semaphore_signal(barrier, inc=1, device_id={"dp": lax.rem(me + o, n)}, device_id_type=MESH)

    tok = tok_ref[...].astype(F32)
    scale = lax.rsqrt(jnp.sum(tok * tok, axis=-1, keepdims=True) * (1.0 / width) + epsilon)
    normed = tok * scale * gain_ref[...]
    for d in range(n):
        sbuf[d] = normed[:, d * depth : (d + 1) * depth].astype(BF16)
    pl.semaphore_wait(barrier, n - 1)

    def spread(o):
        to = lax.rem(me + o, n)
        return pltpu.make_async_remote_copy(
            src_ref=sbuf.at[to], dst_ref=rbuf.at[me], send_sem=s1.at[o], recv_sem=r1.at[o],
            device_id={"dp": to}, device_id_type=MESH)

    def arrive(o):
        source = lax.rem(me + n - o, n)
        return pltpu.make_async_remote_copy(
            src_ref=sbuf.at[source], dst_ref=rbuf.at[source], send_sem=s1.at[o], recv_sem=r1.at[o],
            device_id={"dp": source}, device_id_type=MESH)

    for o in range(1, n):
        spread(o).start()
    rbuf[me] = sbuf[me]
    for load in loads:
        load.wait()
    for o in range(1, n):
        arrive(o).wait_recv()
    x = rbuf[...].reshape(n * rows, depth)

    def give(o, c):
        to = lax.rem(me + o, n)
        span = pl.ds(c * chunk, chunk)
        return pltpu.make_async_remote_copy(
            src_ref=psend.at[to, :, span], dst_ref=precv.at[me, :, span],
            send_sem=s2.at[o, c], recv_sem=r2.at[o, c],
            device_id={"dp": to}, device_id_type=MESH)

    def take(o, c):
        source = lax.rem(me + n - o, n)
        span = pl.ds(c * chunk, chunk)
        return pltpu.make_async_remote_copy(
            src_ref=psend.at[source, :, span], dst_ref=precv.at[source, :, span],
            send_sem=s2.at[o, c], recv_sem=r2.at[o, c],
            device_id={"dp": source}, device_id_type=MESH)

    for c in range(chunks):
        part = jnp.dot(x, w[:, c * chunk : (c + 1) * chunk], preferred_element_type=F32)
        psend[:, :, c * chunk : (c + 1) * chunk] = part.astype(BF16).reshape(n, rows, chunk)
        for o in range(1, n):
            give(o, c).start()
    precv[me] = psend[me]

    pieces = []
    for c in range(chunks):
        for o in range(1, n):
            take(o, c).wait_recv()
        total = precv[0, :, c * chunk : (c + 1) * chunk].astype(F32)
        for d in range(1, n):
            total = total + precv[d, :, c * chunk : (c + 1) * chunk].astype(F32)
        pieces.append(total)
    joined = pieces[0] if chunks == 1 else jnp.concatenate(pieces, axis=1)

    cos_part = cos_ref[...]
    sin_part = sin_ref[...]

    def head(block, gain):
        mean = jnp.mean(block * block, axis=-1, keepdims=True)
        block = block * lax.rsqrt(mean + epsilon) * gain
        return block * cos_part + pltpu.roll(block, HD // 2, 1) * sin_part

    heads, groups = qc // HD, kc // HD
    per = heads // groups
    for g in range(groups):
        at = qc + g * HD
        key = head(joined[:, at : at + HD], kg_ref[...]).astype(BF16)
        value = joined[:, at + kc : at + kc + HD].astype(BF16)
        nk_out[:, g * HD : (g + 1) * HD] = key
        nv_out[:, g * HD : (g + 1) * HD] = value
        for r in range(per):
            h = g * per + r
            query = head(joined[:, h * HD : (h + 1) * HD], qg_ref[...]) * QPRE ** (-0.5)
            q_out[:, h, :] = query.astype(BF16).astype(F32)
            kx_out[:, h, :] = key.astype(F32)
            vx_out[:, h, :] = value.astype(F32)

    for o in range(1, n):
        spread(o).wait_send()
        for c in range(chunks):
            give(o, c).wait_send()


def attend_kernel(
    len_ref, q_ref, kx_ref, vx_ref, kc_ref, vc_ref, out_ref,
    kbuf, vbuf, scores, weights, mixed, ksem, vsem,
):
    batch, heads, _ = q_ref.shape
    ctx, kv = kbuf.shape[1], kbuf.shape[2]
    groups = kv // HD
    per = heads // groups
    most = ctx // SLOTS

    def copies(b, j):
        span = pl.ds(pl.multiple_of(j * SLOTS, SLOTS), SLOTS)
        return (
            pltpu.make_async_copy(kc_ref.at[b, span], kbuf.at[b, span], ksem.at[b, j]),
            pltpu.make_async_copy(vc_ref.at[b, span], vbuf.at[b, span], vsem.at[b, j]),
        )

    def blocks(b):
        return (len_ref[b] + SLOTS - 1) // SLOTS

    for which in range(2):
        @pl.loop(0, batch)
        def _(b):
            @pl.loop(0, blocks(b))
            def _(j):
                copies(b, j)[which].start()

    row = lax.broadcasted_iota(jnp.int32, (heads, HD), 0) // per

    @pl.loop(0, batch)
    def _(b):
        q8 = q_ref[b]
        spreadq = jnp.concatenate(
            [jnp.where(row == g, q8, 0.0) for g in range(groups)], axis=1).astype(BF16)
        count = blocks(b)
        for size in range(1, most + 1):
            @pl.when(count == size)
            def _():
                for j in range(size):
                    copies(b, j)[0].wait()
                    scores[b, :, j * SLOTS : (j + 1) * SLOTS] = lax.dot_general(
                        spreadq, kbuf[b, j * SLOTS : (j + 1) * SLOTS, :],
                        (((1,), (1,)), ((), ())), preferred_element_type=F32)

    slot = lax.broadcasted_iota(jnp.int32, (heads, ctx), 1)

    @pl.loop(0, batch)
    def _(b):
        own = jnp.sum(q_ref[b] * kx_ref[b], axis=-1, keepdims=True)
        usable = slot < len_ref[b]
        s = jnp.where(usable, scores[b], -jnp.inf)
        largest = jnp.maximum(jnp.max(s, axis=-1, keepdims=True), own)
        w = jnp.exp(s - largest)
        w_own = jnp.exp(own - largest)
        total = jnp.sum(w, axis=-1, keepdims=True) + w_own
        wb = w.astype(BF16)
        count = blocks(b)
        mine = w_own.astype(BF16).astype(F32) * vx_ref[b]
        for size in range(1, most + 1):
            @pl.when(count == size)
            def _():
                for j in range(size):
                    copies(b, j)[1].wait()
                mix = jnp.dot(wb[:, : size * SLOTS], vbuf[b, : size * SLOTS, :],
                              preferred_element_type=F32)
                got = mine
                for g in range(groups):
                    got = got + jnp.where(row == g, mix[:, g * HD : (g + 1) * HD], 0.0)
                mixed[b] = got / total

    for h in range(heads):
        out_ref[:, h * HD : (h + 1) * HD] = mixed[:, h, :].astype(BF16)


def output_kernel(
    n, m, width, att_ref, wo_ref, y_out,
    w, gath, ps, pr, fs, fr, acc, wsem, s1, r1, s2, r2, s3, r3,
):
    me = lax.axis_index("dp")
    mt = lax.axis_index("tensor")
    rows, depth = att_ref.shape
    cols = wo_ref.shape[1]
    part = rows // m
    load = pltpu.make_async_copy(wo_ref, w, wsem)
    load.start()
    barrier = pltpu.get_barrier_semaphore()
    others = [(a, b) for a in range(n) for b in range(m) if (a, b) != (0, 0)]

    def place(a, b):
        return {"dp": lax.rem(me + a, n), "tensor": lax.rem(mt + b, m)}

    for a, b in others:
        pl.semaphore_signal(barrier, inc=1, device_id=place(a, b), device_id_type=MESH)
    pl.semaphore_wait(barrier, n * m - 1)

    def gather(o, sender):
        to = lax.rem(me + o, n)
        return pltpu.make_async_remote_copy(
            src_ref=att_ref, dst_ref=gath.at[sender], send_sem=s1.at[o], recv_sem=r1.at[o],
            device_id={"dp": to, "tensor": mt}, device_id_type=MESH)

    for o in range(1, n):
        gather(o, me).start()
    gath[me] = att_ref[...]
    i = lax.broadcasted_iota(jnp.int32, (n * rows, n * rows), 0)
    j = lax.broadcasted_iota(jnp.int32, (n * rows, n * rows), 1)
    t, d, r = i // (n * part), (i // part) % n, i % part
    order = jnp.where(j == d * rows + t * part + r, 1.0, 0.0).astype(BF16)
    load.wait()
    for o in range(1, n):
        gather(o, lax.rem(me + n - o, n)).wait_recv()
    x = gath[...].reshape(n * rows, depth)
    x = jnp.dot(order, x, preferred_element_type=F32).astype(BF16)
    prod = jnp.dot(x, w[...], preferred_element_type=F32)
    ps[...] = prod.astype(BF16).reshape(m, n * part, cols)

    def reduce(o, slot, sender):
        to = lax.rem(mt + o, m)
        return pltpu.make_async_remote_copy(
            src_ref=ps.at[slot], dst_ref=pr.at[sender], send_sem=s2.at[o], recv_sem=r2.at[o],
            device_id={"dp": me, "tensor": to}, device_id_type=MESH)

    for o in range(1, m):
        to = lax.rem(mt + o, m)
        reduce(o, to, mt).start()
    pr[mt] = ps[mt]
    for o in range(1, m):
        source = lax.rem(mt + m - o, m)
        reduce(o, source, source).wait_recv()
    total = pr[0].astype(F32)
    for k in range(1, m):
        total = total + pr[k].astype(F32)
    for d in range(n):
        fs[d] = total[d * part : (d + 1) * part, :].astype(BF16)

    def final(a, b, slot, st, sd):
        return pltpu.make_async_remote_copy(
            src_ref=fs.at[slot], dst_ref=fr.at[st, sd], send_sem=s3.at[a, b], recv_sem=r3.at[a, b],
            device_id=place(a, b), device_id_type=MESH)

    for a, b in others:
        final(a, b, lax.rem(me + a, n), mt, me).start()
    fr[mt, me] = fs[me]
    for a, b in others:
        sd, st = lax.rem(me + n - a, n), lax.rem(mt + m - b, m)
        final(a, b, sd, st, sd).wait_recv()
    for t in range(m):
        for d in range(n):
            acc[d, t * part : (t + 1) * part, :] = fr[t, d].astype(F32)
    square = jnp.zeros((rows, 1), F32)
    for d in range(n):
        square = square + jnp.sum(acc[d] * acc[d], axis=-1, keepdims=True)
    scale = lax.rsqrt(square * (1.0 / width) + epsilon)
    for d in range(n):
        y_out[d] = acc[d] * scale

    for o in range(1, n):
        gather(o, me).wait_send()
    for o in range(1, m):
        reduce(o, lax.rem(mt + o, m), mt).wait_send()
    for a, b in others:
        final(a, b, lax.rem(me + a, n), mt, me).wait_send()


def per_device(
    n, m, tokens, lengths, positions, in_gain, q_weight, k_weight, v_weight, q_gain, k_gain,
    key_cache, value_cache, out_weight, post_gain,
):
    rows, width = tokens.shape
    depth, qc = q_weight.shape
    kc = k_weight.shape[1]
    cols = qc + 2 * kc
    chunks = cols // min(512, cols)
    heads = qc // HD
    ctx = key_cache.shape[1]
    half = HD // 2
    exponent = jnp.arange(half, dtype=F32) * (2.0 / HD)
    frequency = jnp.power(rope_base, -exponent)
    angles = (positions.astype(F32) / rope_factor)[:, None] * frequency[None, :]
    cos_half, sin_half = jnp.cos(angles), jnp.sin(angles)
    cos_part = jnp.concatenate([cos_half, cos_half], axis=1)
    sin_part = jnp.concatenate([-sin_half, sin_half], axis=1)

    full = pl.BlockSpec(memory_space=VMEM)
    anywhere = pl.BlockSpec(memory_space=pl.ANY)
    dma = pltpu.SemaphoreType.DMA
    q8, kx, vx, new_keys, new_values = pl.pallas_call(
        functools.partial(project_kernel, n),
        name="project",
        out_shape=[
            jax.ShapeDtypeStruct((rows, heads, HD), F32),
            jax.ShapeDtypeStruct((rows, heads, HD), F32),
            jax.ShapeDtypeStruct((rows, heads, HD), F32),
            jax.ShapeDtypeStruct((rows, kc), BF16),
            jax.ShapeDtypeStruct((rows, kc), BF16),
        ],
        in_specs=[full] * 6 + [anywhere] * 3,
        out_specs=[full] * 5,
        scratch_shapes=[
            VMEM((depth, cols), BF16),
            VMEM((n, rows, depth), BF16),
            VMEM((n, rows, depth), BF16),
            VMEM((n, rows, cols), BF16),
            VMEM((n, rows, cols), BF16),
            dma((3,)), dma((n,)), dma((n,)), dma((n, chunks)), dma((n, chunks)),
        ],
        compiler_params=pltpu.CompilerParams(
            collective_id=0, has_side_effects=True, vmem_limit_bytes=40 * 2**20),
    )(tokens, in_gain[None, :], cos_part, sin_part, q_gain[None, :], k_gain[None, :],
      q_weight, k_weight, v_weight)

    attended = pl.pallas_call(
        attend_kernel,
        name="attend",
        out_shape=jax.ShapeDtypeStruct((rows, qc), BF16),
        in_specs=[pl.BlockSpec(memory_space=pltpu.SMEM)] + [full] * 3 + [anywhere] * 2,
        out_specs=full,
        scratch_shapes=[
            VMEM((rows, ctx, kc), BF16),
            VMEM((rows, ctx, kc), BF16),
            VMEM((rows, heads, ctx), F32),
            VMEM((rows, heads, ctx), BF16),
            VMEM((rows, heads, HD), F32),
            dma((rows, ctx // SLOTS)), dma((rows, ctx // SLOTS)),
        ],
        compiler_params=pltpu.CompilerParams(vmem_limit_bytes=56 * 2**20),
    )(lengths, q8, kx, vx, key_cache, value_cache)

    ocols = out_weight.shape[1]
    part = rows // m
    y = pl.pallas_call(
        functools.partial(output_kernel, n, m, width),
        name="output",
        out_shape=jax.ShapeDtypeStruct((n, rows, ocols), F32),
        in_specs=[full, anywhere],
        out_specs=full,
        scratch_shapes=[
            VMEM((qc, ocols), BF16),
            VMEM((n, rows, qc), BF16),
            VMEM((m, n * part, ocols), BF16),
            VMEM((m, n * part, ocols), BF16),
            VMEM((n, part, ocols), BF16),
            VMEM((m, n, part, ocols), BF16),
            VMEM((n, rows, ocols), F32),
            dma, dma((n,)), dma((n,)), dma((m,)), dma((m,)), dma((n, m)), dma((n, m)),
        ],
        compiler_params=pltpu.CompilerParams(
            collective_id=1, has_side_effects=True, vmem_limit_bytes=40 * 2**20),
    )(attended, out_weight)
    y = jnp.swapaxes(y, 0, 1).reshape(rows, width)
    hidden_out = (tokens.astype(F32) + y * post_gain).astype(BF16)
    return (hidden_out, new_keys, new_values)


def solution(mesh):
    n, m = mesh.shape["dp"], mesh.shape["tensor"]
    return jax.shard_map(
        functools.partial(per_device, n, m),
        mesh=mesh,
        in_specs=(
            P("dp", None),
            P("dp"),
            P("dp"),
            P(),
            P("dp", "tensor"),
            P("dp", "tensor"),
            P("dp", "tensor"),
            P(),
            P(),
            P("dp", None, "tensor"),
            P("dp", None, "tensor"),
            P("tensor", "dp"),
            P(),
        ),
        out_specs=(P("dp", None), P("dp", "tensor"), P("dp", "tensor")),
        check_vma=False,
    )
```

```python
import functools

import jax
import jax.numpy as jnp
from jax import lax
from jax.experimental import pallas as pl
from jax.experimental.pallas import tpu as pltpu
from jax.sharding import PartitionSpec as P

HD = 128
QPRE = 168
SLOTS = 256
FULL = 67043328

epsilon = 1e-06
rope_base = 1000000.0
rope_factor = 8.0

MESH = pl.DeviceIdType.MESH
VMEM = pltpu.VMEM
F32 = jnp.float32
BF16 = jnp.bfloat16


def project_kernel(
    n, tok_ref, gain_ref, cos_ref, sin_ref, qg_ref, kg_ref, wq_ref, wk_ref, wv_ref,
    qkv_out,
    tok_v, gain_v, qg_v, kg_v, w, sbuf, rbuf, psend, precv, lsem, wsem, s1, r1, s2, r2,
):
    me = lax.axis_index("dp")
    rows, width = tok_ref.shape
    depth = wq_ref.shape[0]
    qc, kc = wq_ref.shape[1], wk_ref.shape[1]
    cols = qc + 2 * kc
    chunk = min(512, cols)
    chunks = cols // chunk

    loads = [
        pltpu.make_async_copy(wq_ref, w.at[:, pl.ds(0, qc)], wsem.at[0]),
        pltpu.make_async_copy(wk_ref, w.at[:, pl.ds(qc, kc)], wsem.at[1]),
        pltpu.make_async_copy(wv_ref, w.at[:, pl.ds(qc + kc, kc)], wsem.at[2]),
    ]
    small = [
        pltpu.make_async_copy(tok_ref, tok_v, lsem.at[0]),
        pltpu.make_async_copy(gain_ref, gain_v, lsem.at[1]),
        pltpu.make_async_copy(qg_ref, qg_v, lsem.at[2]),
        pltpu.make_async_copy(kg_ref, kg_v, lsem.at[3]),
    ]
    for load in small + loads:
        load.start()
    barrier = pltpu.get_barrier_semaphore()
    for o in range(1, n):
        pl.semaphore_signal(barrier, inc=1, device_id={"dp": lax.rem(me + o, n)}, device_id_type=MESH)

    for load in small:
        load.wait()
    tok = tok_v[...].astype(F32)
    scale = lax.rsqrt(jnp.sum(tok * tok, axis=-1, keepdims=True) * (1.0 / width) + epsilon)
    normed = jnp.concatenate([
        tok[:, k * HD : (k + 1) * HD] * scale * gain_v[k : k + 1, :] for k in range(width // HD)
    ], axis=1)
    for d in range(n):
        sbuf[d] = normed[:, d * depth : (d + 1) * depth].astype(BF16)
    pl.semaphore_wait(barrier, n - 1)

    def spread(o):
        to = lax.rem(me + o, n)
        return pltpu.make_async_remote_copy(
            src_ref=sbuf.at[to], dst_ref=rbuf.at[me], send_sem=s1.at[o], recv_sem=r1.at[o],
            device_id={"dp": to}, device_id_type=MESH)

    def arrive(o):
        source = lax.rem(me + n - o, n)
        return pltpu.make_async_remote_copy(
            src_ref=sbuf.at[source], dst_ref=rbuf.at[source], send_sem=s1.at[o], recv_sem=r1.at[o],
            device_id={"dp": source}, device_id_type=MESH)

    for o in range(1, n):
        spread(o).start()
    rbuf[me] = sbuf[me]
    for load in loads:
        load.wait()
    for o in range(1, n):
        arrive(o).wait_recv()
    x = rbuf[...].reshape(n * rows, depth)

    def give(o, c):
        to = lax.rem(me + o, n)
        span = pl.ds(c * chunk, chunk)
        return pltpu.make_async_remote_copy(
            src_ref=psend.at[to, :, span], dst_ref=precv.at[me, :, span],
            send_sem=s2.at[o, c], recv_sem=r2.at[o, c],
            device_id={"dp": to}, device_id_type=MESH)

    def take(o, c):
        source = lax.rem(me + n - o, n)
        span = pl.ds(c * chunk, chunk)
        return pltpu.make_async_remote_copy(
            src_ref=psend.at[source, :, span], dst_ref=precv.at[source, :, span],
            send_sem=s2.at[o, c], recv_sem=r2.at[o, c],
            device_id={"dp": source}, device_id_type=MESH)

    for c in range(chunks):
        part = jnp.dot(x, w[:, c * chunk : (c + 1) * chunk], preferred_element_type=F32)
        psend[:, :, c * chunk : (c + 1) * chunk] = part.astype(BF16).reshape(n, rows, chunk)
        for o in range(1, n):
            give(o, c).start()
    precv[me] = psend[me]

    pieces = []
    for c in range(chunks):
        for o in range(1, n):
            take(o, c).wait_recv()
        total = precv[0, :, c * chunk : (c + 1) * chunk].astype(F32)
        for d in range(1, n):
            total = total + precv[d, :, c * chunk : (c + 1) * chunk].astype(F32)
        pieces.append(total)
    joined = pieces[0] if chunks == 1 else jnp.concatenate(pieces, axis=1)

    cos_part = cos_ref[...]
    sin_part = sin_ref[...]

    def head(block, gain):
        mean = jnp.mean(block * block, axis=-1, keepdims=True)
        block = block * lax.rsqrt(mean + epsilon) * gain
        return block * cos_part + pltpu.roll(block, HD // 2, 1) * sin_part

    heads, groups = qc // HD, kc // HD
    per = heads // groups
    for g in range(groups):
        at = qc + g * HD
        key = head(joined[:, at : at + HD], kg_v[...]).astype(BF16)
        value = joined[:, at + kc : at + kc + HD].astype(BF16)
        for r in range(per):
            h = g * per + r
            query = head(joined[:, h * HD : (h + 1) * HD], qg_v[...]) * QPRE ** (-0.5)
            qkv_out[0, :, h, :] = query.astype(BF16).astype(F32)
            qkv_out[1, :, h, :] = key.astype(F32)
            qkv_out[2, :, h, :] = value.astype(F32)

    for o in range(1, n):
        spread(o).wait_send()
        for c in range(chunks):
            give(o, c).wait_send()


def attend_kernel(
    len_ref, qkv_ref, kc_ref, vc_ref, out_ref, nk_out, nv_out,
    qkv_v, kbuf, vbuf, scores, weights, mixed, owns, sums, qsem, ksem, vsem,
):
    _, batch, heads, _ = qkv_ref.shape
    fetch = pltpu.make_async_copy(qkv_ref, qkv_v, qsem)
    fetch.start()
    q_ref, kx_ref, vx_ref = qkv_v.at[0], qkv_v.at[1], qkv_v.at[2]
    ctx, kv = kbuf.shape[1], kbuf.shape[2]
    groups = kv // HD
    per = heads // groups
    most = ctx // SLOTS

    def copies(b, j):
        span = pl.ds(pl.multiple_of(j * SLOTS, SLOTS), SLOTS)
        return (
            pltpu.make_async_copy(kc_ref.at[b, span], kbuf.at[b, span], ksem.at[b, j]),
            pltpu.make_async_copy(vc_ref.at[b, span], vbuf.at[b, span], vsem.at[b, j]),
        )

    def blocks(b):
        return (len_ref[b] + SLOTS - 1) // SLOTS

    for which in range(2):
        @pl.loop(0, batch)
        def _(b):
            @pl.loop(0, blocks(b))
            def _(j):
                copies(b, j)[which].start()

    fetch.wait()
    row = lax.broadcasted_iota(jnp.int32, (heads, HD), 0) // per

    @pl.loop(0, batch)
    def _(b):
        q8 = q_ref[b]
        spreadq = jnp.concatenate(
            [jnp.where(row == g, q8, 0.0) for g in range(groups)], axis=1).astype(BF16)
        count = blocks(b)
        for size in range(1, most + 1):
            @pl.when(count == size)
            def _():
                for j in range(size):
                    copies(b, j)[0].wait()
                scores[b, :, : size * SLOTS] = lax.dot_general(
                    spreadq, kbuf[b, : size * SLOTS, :],
                    (((1,), (1,)), ((), ())), preferred_element_type=F32)

    slot = lax.broadcasted_iota(jnp.int32, (heads, ctx), 1)
    for b in range(batch):
        own = jnp.sum(q_ref[b] * kx_ref[b], axis=-1, keepdims=True)
        s = jnp.where(slot < len_ref[b], scores[b], -jnp.inf)
        largest = jnp.maximum(jnp.max(s, axis=-1, keepdims=True), own)
        w = jnp.exp(s - largest)
        w_own = jnp.exp(own - largest)
        sums[b] = jnp.broadcast_to(jnp.sum(w, axis=-1, keepdims=True) + w_own, (heads, HD))
        owns[b] = w_own.astype(BF16).astype(F32) * vx_ref[b]
        weights[b] = w.astype(BF16)

    @pl.loop(0, batch)
    def _(b):
        count = blocks(b)
        for size in range(1, most + 1):
            @pl.when(count == size)
            def _():
                for j in range(size):
                    copies(b, j)[1].wait()
                mix = jnp.dot(weights[b, :, : size * SLOTS], vbuf[b, : size * SLOTS, :],
                              preferred_element_type=F32)
                got = mix[:, :HD]
                for g in range(1, groups):
                    got = jnp.where(row == g, mix[:, g * HD : (g + 1) * HD], got)
                mixed[b] = got

    mixed[...] = (mixed[...] + owns[...]) / sums[...]
    for h in range(heads):
        out_ref[:, h * HD : (h + 1) * HD] = mixed[:, h, :].astype(BF16)
    for g in range(groups):
        nk_out[:, g * HD : (g + 1) * HD] = kx_ref[:, g * per, :].astype(BF16)
        nv_out[:, g * HD : (g + 1) * HD] = vx_ref[:, g * per, :].astype(BF16)


def output_kernel(
    n, m, width, att_hbm, wo_ref, y_out,
    att_ref, w, gath, ps, pr, fs, fr, acc, asem, wsem, s1, r1, s2, r2, s3, r3,
):
    me = lax.axis_index("dp")
    mt = lax.axis_index("tensor")
    rows, depth = att_ref.shape
    cols = wo_ref.shape[0]
    part = rows // m
    local = pltpu.make_async_copy(att_hbm, att_ref, asem)
    local.start()
    load = pltpu.make_async_copy(wo_ref, w, wsem)
    load.start()
    barrier = pltpu.get_barrier_semaphore()
    others = [(a, b) for a in range(n) for b in range(m) if (a, b) != (0, 0)]

    def place(a, b):
        return {"dp": lax.rem(me + a, n), "tensor": lax.rem(mt + b, m)}

    for a, b in others:
        pl.semaphore_signal(barrier, inc=1, device_id=place(a, b), device_id_type=MESH)
    local.wait()
    pl.semaphore_wait(barrier, n * m - 1)

    def gather(o, sender):
        to = lax.rem(me + o, n)
        return pltpu.make_async_remote_copy(
            src_ref=att_ref, dst_ref=gath.at[sender], send_sem=s1.at[o], recv_sem=r1.at[o],
            device_id={"dp": to, "tensor": mt}, device_id_type=MESH)

    for o in range(1, n):
        gather(o, me).start()
    gath[me] = att_ref[...]
    i = lax.broadcasted_iota(jnp.int32, (n * rows, n * rows), 0)
    j = lax.broadcasted_iota(jnp.int32, (n * rows, n * rows), 1)
    t, d, r = i // (n * part), (i // part) % n, i % part
    order = jnp.where(j == d * rows + t * part + r, 1.0, 0.0).astype(BF16)
    load.wait()
    for o in range(1, n):
        gather(o, lax.rem(me + n - o, n)).wait_recv()
    x = gath[...].reshape(n * rows, depth)
    x = jnp.dot(order, x, preferred_element_type=F32).astype(BF16)
    prod = lax.dot_general(x, w[...], (((1,), (1,)), ((), ())), preferred_element_type=F32)
    ps[...] = prod.astype(BF16).reshape(m, n * part, cols)

    def reduce(o, slot, sender):
        to = lax.rem(mt + o, m)
        return pltpu.make_async_remote_copy(
            src_ref=ps.at[slot], dst_ref=pr.at[sender], send_sem=s2.at[o], recv_sem=r2.at[o],
            device_id={"dp": me, "tensor": to}, device_id_type=MESH)

    for o in range(1, m):
        to = lax.rem(mt + o, m)
        reduce(o, to, mt).start()
    pr[mt] = ps[mt]
    for o in range(1, m):
        source = lax.rem(mt + m - o, m)
        reduce(o, source, source).wait_recv()
    total = pr[0].astype(F32)
    for k in range(1, m):
        total = total + pr[k].astype(F32)
    for d in range(n):
        fs[d] = total[d * part : (d + 1) * part, :].astype(BF16)

    def final(a, b, slot, st, sd):
        return pltpu.make_async_remote_copy(
            src_ref=fs.at[slot], dst_ref=fr.at[st, sd], send_sem=s3.at[a, b], recv_sem=r3.at[a, b],
            device_id=place(a, b), device_id_type=MESH)

    for a, b in others:
        final(a, b, lax.rem(me + a, n), mt, me).start()
    fr[mt, me] = fs[me]
    for a, b in others:
        sd, st = lax.rem(me + n - a, n), lax.rem(mt + m - b, m)
        final(a, b, sd, st, sd).wait_recv()
    for t in range(m):
        for d in range(n):
            acc[d, t * part : (t + 1) * part, :] = fr[t, d].astype(F32)
    square = jnp.zeros((rows, 1), F32)
    for d in range(n):
        square = square + jnp.sum(acc[d] * acc[d], axis=-1, keepdims=True)
    scale = lax.rsqrt(square * (1.0 / width) + epsilon)
    for d in range(n):
        y_out[d] = acc[d] * scale

    for o in range(1, n):
        gather(o, me).wait_send()
    for o in range(1, m):
        reduce(o, lax.rem(mt + o, m), mt).wait_send()
    for a, b in others:
        final(a, b, lax.rem(me + a, n), mt, me).wait_send()


def per_device(
    n, m, tokens, lengths, positions, in_gain, q_weight, k_weight, v_weight, q_gain, k_gain,
    key_cache, value_cache, out_weight, post_gain,
):
    rows, width = tokens.shape
    depth, qc = q_weight.shape
    kc = k_weight.shape[1]
    cols = qc + 2 * kc
    chunks = cols // min(512, cols)
    heads = qc // HD
    ctx = key_cache.shape[1]
    half = HD // 2
    exponent = jnp.arange(half, dtype=F32) * (2.0 / HD)
    frequency = jnp.power(rope_base, -exponent)
    angles = (positions.astype(F32) / rope_factor)[:, None] * frequency[None, :]
    cos_half, sin_half = jnp.cos(angles), jnp.sin(angles)
    cos_part = jnp.concatenate([cos_half, cos_half], axis=1)
    sin_part = jnp.concatenate([-sin_half, sin_half], axis=1)

    full = pl.BlockSpec(memory_space=VMEM)
    anywhere = pl.BlockSpec(memory_space=pltpu.HBM)
    dma = pltpu.SemaphoreType.DMA
    qkv = pl.pallas_call(
        functools.partial(project_kernel, n),
        name="project",
        out_shape=jax.ShapeDtypeStruct((3, rows, heads, HD), F32),
        in_specs=[anywhere] * 2 + [full] * 2 + [anywhere] * 5,
        out_specs=full,
        scratch_shapes=[
            VMEM((rows, width), BF16),
            VMEM((width // HD, HD), F32),
            VMEM((1, HD), F32),
            VMEM((1, HD), F32),
            VMEM((depth, cols), BF16),
            VMEM((n, rows, depth), BF16),
            VMEM((n, rows, depth), BF16),
            VMEM((n, rows, cols), BF16),
            VMEM((n, rows, cols), BF16),
            dma((4,)), dma((3,)), dma((n,)), dma((n,)), dma((n, chunks)), dma((n, chunks)),
        ],
        compiler_params=pltpu.CompilerParams(
            collective_id=0, has_side_effects=True, vmem_limit_bytes=FULL),
    )(tokens, in_gain.reshape(width // HD, HD), cos_part, sin_part, q_gain[None, :], k_gain[None, :],
      q_weight, k_weight, v_weight)

    attended, new_keys, new_values = pl.pallas_call(
        attend_kernel,
        name="attend",
        out_shape=[
            jax.ShapeDtypeStruct((rows, qc), BF16),
            jax.ShapeDtypeStruct((rows, kc), BF16),
            jax.ShapeDtypeStruct((rows, kc), BF16),
        ],
        in_specs=[pl.BlockSpec(memory_space=pltpu.SMEM)] + [anywhere] * 3,
        out_specs=[full] * 3,
        scratch_shapes=[
            VMEM((3, rows, heads, HD), F32),
            VMEM((rows, ctx, kc), BF16),
            VMEM((rows, ctx, kc), BF16),
            VMEM((rows, heads, ctx), F32),
            VMEM((rows, heads, ctx), BF16),
            VMEM((rows, heads, HD), F32),
            VMEM((rows, heads, HD), F32),
            VMEM((rows, heads, HD), F32),
            dma, dma((rows, ctx // SLOTS)), dma((rows, ctx // SLOTS)),
        ],
        compiler_params=pltpu.CompilerParams(vmem_limit_bytes=FULL),
    )(lengths, qkv, key_cache, value_cache)

    ocols = out_weight.shape[1]
    part = rows // m
    result = 4 * n * rows * (-(-ocols // HD) * HD)
    y = pl.pallas_call(
        functools.partial(output_kernel, n, m, width),
        name="output",
        out_shape=jax.ShapeDtypeStruct((n, rows, ocols), F32),
        in_specs=[anywhere, anywhere],
        out_specs=full,
        scratch_shapes=[
            VMEM((rows, qc), BF16),
            VMEM((ocols, qc), BF16),
            VMEM((n, rows, qc), BF16),
            VMEM((m, n * part, ocols), BF16),
            VMEM((m, n * part, ocols), BF16),
            VMEM((n, part, ocols), BF16),
            VMEM((m, n, part, ocols), BF16),
            VMEM((n, rows, ocols), F32),
            dma, dma, dma((n,)), dma((n,)), dma((m,)), dma((m,)), dma((n, m)), dma((n, m)),
        ],
        compiler_params=pltpu.CompilerParams(
            collective_id=1, has_side_effects=True, vmem_limit_bytes=FULL - result + 44 * 1024),
    )(attended, out_weight.T)
    y = jnp.swapaxes(y, 0, 1).reshape(rows, width)
    hidden_out = (tokens.astype(F32) + y * post_gain).astype(BF16)
    return (hidden_out, new_keys, new_values)


def solution(mesh):
    n, m = mesh.shape["dp"], mesh.shape["tensor"]
    return jax.shard_map(
        functools.partial(per_device, n, m),
        mesh=mesh,
        in_specs=(
            P("dp", None),
            P("dp"),
            P("dp"),
            P(),
            P("dp", "tensor"),
            P("dp", "tensor"),
            P("dp", "tensor"),
            P(),
            P(),
            P("dp", None, "tensor"),
            P("dp", None, "tensor"),
            P("tensor", "dp"),
            P(),
        ),
        out_specs=(P("dp", None), P("dp", "tensor"), P("dp", "tensor")),
        check_vma=False,
    )
```
